32 devices in a mesh: span: 4 (over y, x), model: 8 (over z, core).
Axes of the slice: x: 2, y: 2, z: 4, core: 2. Of those that a mesh axis runs over, the one named last changes fastest.
Arguments:
- latents: bfloat16 [4, 2048, 512], P(None, ('span', 'model')), may hold values from -6 to 6
- rotary_rows: bfloat16 [4, 2048, 64], P(None, ('span', 'model')), may hold values from -6 to 6
- latent_gain: float32 [512], replicated, may hold values from 0.25 to 1.75
- key_up: bfloat16 [512, 16, 128], P(None, 'model'), may hold values from -0.25 to 0.25
- value_up: bfloat16 [512, 16, 128], P(None, 'model'), may hold values from -0.25 to 0.25
Outputs:
- decode_keys: bfloat16 [4, 16, 192, 2048], P('span', 'model')
- decode_values: bfloat16 [4, 2048, 16, 128], P('span', None, 'model')
The draws below stay inside these ranges and needn't reach their ends.
All inputs are finite; a program needn't handle non-finite values.
Results may differ from the reference program's by a relative error of at most 0.0049.
Values may be sent and summed in bfloat16 or wider, within the bound.
A program may use at most 64 MiB of HBM per device.

```python
import jax
import jax.numpy as jnp
from jax import lax

BATCH = 4
LENGTH = 2048
HEADS = 16
LATENT = 512
KEY_PART = 128
ROTARY = 64
VALUE_SIZE = 128


def block_levels(own_key, dims, pieces, smallest, high):
    factor_of, own = 1.0, jax.random.fold_in(own_key, 6)
    for dim, shards_of in pieces:
        heights = jnp.exp(jax.random.uniform(jax.random.fold_in(own, dim), (shards_of,), jnp.float32, smallest / len(pieces), high / len(pieces)))
        factor_of = factor_of * jnp.repeat(heights, dims[dim] // shards_of).reshape([-1 if axis == dim else 1 for axis in range(len(dims))])
    return factor_of


def normal_values(own_key, shape, scale, most, cuts=(), dtype=jnp.bfloat16):
    loudness = block_levels(own_key, shape, cuts, -0.22, 0.18) if cuts else 1.0
    entries = jax.random.normal(own_key, shape, jnp.float32) * scale * loudness
    return jnp.minimum(jnp.maximum(entries, -most), most).astype(dtype)


def setup_inputs(seed: int = 0) -> dict:
    streams_of = jax.random.split(jax.random.key(seed), 6)
    return {
        "latents": normal_values(streams_of[0], (BATCH, LENGTH, LATENT), 1.0, 6.0, ((1, 32),)),
        "rotary_rows": normal_values(streams_of[1], (BATCH, LENGTH, ROTARY), 1.0, 6.0, ((1, 32),)),
        "latent_gain": jnp.clip(1.0 + 0.15 * jax.random.normal(streams_of[2], (LATENT,), jnp.float32), 0.25, 1.75),
        "key_up": normal_values(streams_of[3], (LATENT, HEADS, KEY_PART), LATENT ** -0.5, 0.25, ((1, 8),)),
        "value_up": normal_values(streams_of[4], (LATENT, HEADS, VALUE_SIZE), LATENT ** -0.5, 0.25, ((1, 8),)),
    }


def scale_rows(vectors, row_gain):
    return vectors * lax.rsqrt(lax.optimization_barrier(jnp.mean(vectors * vectors, axis=-1, keepdims=True)) + 1e-06) * row_gain

def reference(latents, rotary_rows, latent_gain, key_up, value_up):
    rows_ready = scale_rows(latents.astype(jnp.float32), latent_gain).astype(jnp.bfloat16)
    rows_ready = lax.optimization_barrier(rows_ready)

    def expand_one(one):
        rows_one, rotary_one = one
        wide_keys = jnp.einsum('tr,rhk->thk', rows_one.astype(jnp.float32), key_up.astype(jnp.float32)).astype(jnp.bfloat16)
        shared = jnp.broadcast_to(rotary_one[:, None], (LENGTH, HEADS, ROTARY))
        wide_values = jnp.einsum('tr,rhk->thk', rows_one.astype(jnp.float32), value_up.astype(jnp.float32)).astype(jnp.bfloat16)
        return (jnp.concatenate([wide_keys, shared], axis=-1), wide_values)
    decode_keys, decode_values = lax.map(expand_one, (rows_ready, rotary_rows))
    decode_keys = jnp.transpose(decode_keys, (0, 2, 3, 1))
    return (decode_keys, decode_values)
```

```python
import functools

import jax
import jax.numpy as jnp
from jax import lax
from jax.experimental import pallas as pl
from jax.experimental.pallas import tpu as pltpu
from jax.sharding import PartitionSpec as P

CORES = 2
LANES = 128


def gather_expand(
    spans,
    levels,
    latents,
    rotary,
    gain_ref,
    key_up,
    value_up,
    keys_out,
    values_out,
    mine,
    rotary_raw,
    rotary_mine,
    rows,
    turned,
    wide,
    key_weights,
    value_weights,
    mixed,
    local_sem,
    cross_sem,
    up_sem,
    down_sem,
    pair_sem,
    got_sem,
    pair_got_sem,
):
    span = lax.axis_index("span")
    model = lax.axis_index("model")
    level, core = model // CORES, model % CORES
    length, latent = latents.shape[1], latents.shape[2]
    rotary_size = rotary.shape[2]
    half = length // 2
    heads, key_size = keys_out.shape[0], wide.shape[1]
    has_up, has_down = level < levels - 1, level > 0

    def device(to_span, to_level, to_core):
        return {"span": to_span, "model": to_level * CORES + to_core}

    above = device(span, level + 1, core)
    below = device(span, level - 1, core)
    pair = device(span, level, 1 - core)

    def first_row(origin, plane):
        return (origin * levels + plane) * (CORES * length)

    def place(part, origin, plane, of_core):
        start = first_row(origin, plane) + of_core * length
        if part == 0:
            return rows.at[pl.ds(pl.multiple_of(start, length), length)]
        return turned.at[pl.ds(pl.multiple_of(start // 2, half), half)]

    def send(part, origin, plane, source, target, send_sem, recv_sem):
        slot = origin * levels + plane
        here = place(part, origin, plane, core)
        return pltpu.make_async_remote_copy(
            src_ref=here if source is None else source,
            dst_ref=here,
            send_sem=send_sem.at[slot, part],
            recv_sem=recv_sem.at[slot, part],
            device_id=target,
            device_id_type=pl.DeviceIdType.MESH,
        )

    def cross(part, step):
        to_span = lax.rem(span + (spans - step), spans)
        source = mine if part == 0 else rotary_mine
        return pltpu.make_async_remote_copy(
            src_ref=source.at[to_span],
            dst_ref=place(part, span, level, core),
            send_sem=cross_sem.at[step, part],
            recv_sem=got_sem.at[span * levels + level, part],
            device_id=device(to_span, level, core),
            device_id_type=pl.DeviceIdType.MESH,
        )

    def arrived(part, origin, plane):
        send(part, origin, plane, None, pair, pair_sem, got_sem).wait_recv()

    def pair_arrived(origin, plane):
        for part in range(2):
            slot = origin * levels + plane
            there = place(part, origin, plane, 1 - core)
            pltpu.make_async_remote_copy(
                src_ref=there,
                dst_ref=there,
                send_sem=pair_sem.at[slot, part],
                recv_sem=pair_got_sem.at[slot, part],
                device_id=pair,
                device_id_type=pl.DeviceIdType.MESH,
            ).wait_recv()

    barrier = pltpu.get_barrier_semaphore()

    def greet(target):
        pl.semaphore_signal(
            barrier, inc=1, device_id=target, device_id_type=pl.DeviceIdType.MESH
        )

    @pl.when(has_up)
    def _():
        greet(above)

    @pl.when(has_down)
    def _():
        greet(below)

    greet(pair)
    for step in range(1, spans):
        greet(device(lax.rem(span + step, spans), level, core))

    local = [
        pltpu.make_async_copy(latents, mine, local_sem.at[0]),
        pltpu.make_async_copy(rotary, rotary_raw, local_sem.at[1]),
        pltpu.make_async_copy(
            latents.at[span], place(0, span, level, core), local_sem.at[2]
        ),
    ]
    for copy in local:
        copy.start()
    local[1].wait()
    for sequence in range(spans):
        rotary_mine[sequence] = jnp.concatenate(
            [rotary_raw[sequence, :half], rotary_raw[sequence, half:]], axis=1
        )
    place(1, span, level, core)[...] = rotary_mine[span]
    local[0].wait()
    pl.semaphore_wait(
        barrier, spans + has_up.astype(jnp.int32) + has_down.astype(jnp.int32)
    )

    own = (mine.at[span], rotary_mine.at[span])
    for part in range(2):

        @pl.when(has_up)
        def _():
            send(part, span, level, own[part], above, up_sem, got_sem).start()

        @pl.when(has_down)
        def _():
            send(part, span, level, own[part], below, down_sem, got_sem).start()

        for step in range(1, spans):
            cross(part, step).start()
        send(part, span, level, own[part], pair, pair_sem, pair_got_sem).start()

    wide[...] = key_up[...].astype(jnp.float32)
    for head in range(heads):
        weight = wide[pl.ds(head, latent, stride=heads), :] if heads > 1 else wide[...]
        key_weights[head * key_size : (head + 1) * key_size, :] = weight.T.astype(
            jnp.bfloat16
        )
    wide[...] = value_up[...].astype(jnp.float32)
    for head in range(heads):
        weight = wide[pl.ds(head, latent, stride=heads), :] if heads > 1 else wide[...]
        value_weights[:, head * key_size : (head + 1) * key_size] = weight.astype(
            jnp.bfloat16
        )
    local[2].wait()

    def expand(start, count):
        block = rows[pl.ds(pl.multiple_of(start, count), count), :].astype(jnp.float32)
        scale = lax.rsqrt(jnp.mean(block * block, axis=-1, keepdims=True) + 1e-06)
        ready = (block * scale * gain_ref[...]).astype(jnp.bfloat16)
        lanes = pl.ds(pl.multiple_of(start, count), count)
        keys = lax.dot_general(
            key_weights[...],
            ready,
            (((1,), (1,)), ((), ())),
            preferred_element_type=jnp.float32,
        ).astype(jnp.bfloat16)
        packed = turned[
            pl.ds(pl.multiple_of(start // 2, count // 2), count // 2), :
        ].astype(jnp.float32)
        pieces = []
        for first in range(0, count // 2, half):
            piece = packed[first : first + half]
            pieces += [piece, pltpu.roll(piece, rotary_size, 1)]
        shared = jnp.concatenate(pieces, axis=0).T[:rotary_size].astype(jnp.bfloat16)
        for head in range(heads):
            keys_out[head, :key_size, lanes] = keys[
                head * key_size : (head + 1) * key_size
            ]
            keys_out[head, key_size:, lanes] = shared
        values = jnp.dot(
            ready, value_weights[...], preferred_element_type=jnp.float32
        )
        if heads > 1:
            for head in range(heads):
                mixed[pl.ds(head, count, stride=heads), :] = values[
                    :, head * key_size : (head + 1) * key_size
                ]
            values = mixed[...]
        values_out[
            pl.ds(pl.multiple_of(start * heads, count * heads), count * heads), :
        ] = values.astype(jnp.bfloat16)

    chunk = mixed.shape[0] // heads
    early = chunk == CORES * length

    def finish(origin, plane):
        pair_arrived(origin, plane)
        if early:
            expand(first_row(origin, plane), chunk)

    def origin_of(step):
        return lax.rem(span + step, spans)

    def own_level(step, _):
        origin = origin_of(step)
        for part in range(2):
            arrived(part, origin, level)

            @pl.when(has_up)
            def _():
                send(part, origin, level, None, above, up_sem, got_sem).start()

            @pl.when(has_down)
            def _():
                send(part, origin, level, None, below, down_sem, got_sem).start()

            send(part, origin, level, None, pair, pair_sem, pair_got_sem).start()
        finish(origin_of(step - 1), level)
        return 0

    lax.fori_loop(1, spans, own_level, 0)

    def pass_on(step, _):
        away = 1 + step // spans
        origin = origin_of(lax.rem(step, spans))
        for plane, exists, more, target, sem in (
            (level - away, level >= away, has_up, above, up_sem),
            (level + away, level + away < levels, has_down, below, down_sem),
        ):

            @pl.when(exists)
            def _():
                for part in range(2):
                    arrived(part, origin, plane)

                    @pl.when(more)
                    def _():
                        send(part, origin, plane, None, target, sem, got_sem).start()

                    send(part, origin, plane, None, pair, pair_sem, pair_got_sem).start()

        finish_step(step - 1)
        return 0

    def finish_step(step):
        @pl.when(step < 0)
        def _():
            finish(origin_of(spans - 1), level)

        away = 1 + step // spans
        origin = origin_of(lax.rem(step + spans, spans))

        @pl.when((step >= 0) & (level >= away))
        def _():
            finish(origin, level - away)

        @pl.when((step >= 0) & (level + away < levels))
        def _():
            finish(origin, level + away)

    steps = (levels - 1) * spans
    lax.fori_loop(0, steps, pass_on, 0)
    finish_step(steps - 1)

    if not early:

        def late(step, _):
            expand(step * chunk, chunk)
            return 0

        lax.fori_loop(0, rows.shape[0] // chunk, late, 0)

    def drain(slot, _):
        origin, plane = slot // levels, slot % levels
        for part in range(2):

            @pl.when(has_up & (plane <= level))
            def _():
                send(part, origin, plane, None, above, up_sem, got_sem).wait_send()

            @pl.when(has_down & (plane >= level))
            def _():
                send(part, origin, plane, None, below, down_sem, got_sem).wait_send()

            send(part, origin, plane, None, pair, pair_sem, pair_got_sem).wait_send()
        return 0

    lax.fori_loop(0, spans * levels, drain, 0)
    for step in range(1, spans):
        for part in range(2):
            cross(part, step).wait_send()


def shards(spans, levels, latents, rotary_rows, latent_gain, key_up, value_up):
    sequences, length, latent = latents.shape
    rotary_size = rotary_rows.shape[2]
    heads, key_size = key_up.shape[1:]
    total = spans * levels * CORES * length
    chunk = max(CORES * length, LANES)
    vmem = pl.BlockSpec(memory_space=pltpu.VMEM)
    hbm = pl.BlockSpec(memory_space=pl.ANY)
    slots = spans * levels
    sems = pltpu.SemaphoreType.DMA
    keys, values = pl.pallas_call(
        functools.partial(gather_expand, spans, levels),
        out_shape=(
            jax.ShapeDtypeStruct((heads, key_size + rotary_size, total), jnp.bfloat16),
            jax.ShapeDtypeStruct((total * heads, key_size), jnp.bfloat16),
        ),
        in_specs=[hbm, hbm, vmem, vmem, vmem],
        out_specs=(vmem, vmem),
        scratch_shapes=[
            pltpu.VMEM(latents.shape, jnp.bfloat16),
            pltpu.VMEM(rotary_rows.shape, jnp.bfloat16),
            pltpu.VMEM((sequences, length // 2, 2 * rotary_size), jnp.bfloat16),
            pltpu.VMEM((total, latent), jnp.bfloat16),
            pltpu.VMEM((total // 2, 2 * rotary_size), jnp.bfloat16),
            pltpu.VMEM((latent * heads, key_size), jnp.float32),
            pltpu.VMEM((heads * key_size, latent), jnp.bfloat16),
            pltpu.VMEM((latent, heads * key_size), jnp.bfloat16),
            pltpu.VMEM((chunk * heads, key_size), jnp.float32),
            sems((3,)),
            sems((spans, 2)),
            sems((slots, 2)),
            sems((slots, 2)),
            sems((slots, 2)),
            sems((slots, 2)),
            sems((slots, 2)),
        ],
        compiler_params=pltpu.CompilerParams(
            collective_id=0, has_side_effects=True, vmem_limit_bytes=40 * 1024 * 1024
        ),
    )(
        latents,
        rotary_rows,
        latent_gain.reshape(1, latent),
        key_up.reshape(latent * heads, key_size),
        value_up.reshape(latent * heads, key_size),
    )
    return keys[None], values.reshape(1, total, heads, key_size)


def solution(mesh):
    placed = (
        P(None, ("span", "model"), None),
        P(None, ("span", "model"), None),
        P(),
        P(None, "model", None),
        P(None, "model", None),
    )
    spans, levels = mesh.shape["span"], mesh.shape["model"] // CORES
    return jax.shard_map(
        functools.partial(shards, spans, levels),
        mesh=mesh,
        in_specs=placed,
        out_specs=(P("span", "model", None, None), P("span", None, "model", None)),
        check_vma=False,
    )
```

```python
import functools

import jax
import jax.numpy as jnp
from jax import lax
from jax.experimental import pallas as pl
from jax.experimental.pallas import tpu as pltpu
from jax.sharding import PartitionSpec as P

CORES = 2
LANES = 128
VMEM_BYTES = 67043328


def gather_expand(
    spans,
    levels,
    latents,
    rotary,
    gain,
    key_up,
    value_up,
    keys_out,
    values_out,
    mine,
    rotary_raw,
    rotary_mine,
    rows,
    turned,
    gain_ref,
    key_raw,
    value_raw,
    wide,
    key_weights,
    value_weights,
    mixed,
    local_sem,
    cross_sem,
    up_sem,
    down_sem,
    pair_sem,
    got_sem,
    pair_got_sem,
):
    span = lax.axis_index("span")
    model = lax.axis_index("model")
    level, core = model // CORES, model % CORES
    length, latent = latents.shape[1], latents.shape[2]
    rotary_size = rotary.shape[2]
    half = length // 2
    heads, key_size = keys_out.shape[0], wide.shape[1]
    has_up, has_down = level < levels - 1, level > 0

    def device(to_span, to_level, to_core):
        return {"span": to_span, "model": to_level * CORES + to_core}

    above = device(span, level + 1, core)
    below = device(span, level - 1, core)
    pair = device(span, level, 1 - core)

    def first_row(origin, plane):
        return (origin * levels + plane) * (CORES * length)

    def place(part, origin, plane, of_core):
        start = first_row(origin, plane) + of_core * length
        if part == 0:
            return rows.at[pl.ds(pl.multiple_of(start, length), length)]
        return turned.at[pl.ds(pl.multiple_of(start // 2, half), half)]

    def send(part, origin, plane, source, target, send_sem, recv_sem):
        slot = origin * levels + plane
        here = place(part, origin, plane, core)
        return pltpu.make_async_remote_copy(
            src_ref=here if source is None else source,
            dst_ref=here,
            send_sem=send_sem.at[slot, part],
            recv_sem=recv_sem.at[slot, part],
            device_id=target,
            device_id_type=pl.DeviceIdType.MESH,
        )

    def cross(part, step, towards):
        to_span = lax.rem(span + (spans - step), spans)
        source = mine if part == 0 else rotary_mine
        return pltpu.make_async_remote_copy(
            src_ref=source.at[to_span],
            dst_ref=place(part, span, level, core),
            send_sem=cross_sem.at[towards + 1, step, part],
            recv_sem=got_sem.at[span * levels + level, part],
            device_id=device(to_span, level + towards, core),
            device_id_type=pl.DeviceIdType.MESH,
        )

    def arrived(part, origin, plane):
        send(part, origin, plane, None, pair, pair_sem, got_sem).wait_recv()

    def pair_arrived(origin, plane):
        for part in range(2):
            slot = origin * levels + plane
            there = place(part, origin, plane, 1 - core)
            pltpu.make_async_remote_copy(
                src_ref=there,
                dst_ref=there,
                send_sem=pair_sem.at[slot, part],
                recv_sem=pair_got_sem.at[slot, part],
                device_id=pair,
                device_id_type=pl.DeviceIdType.MESH,
            ).wait_recv()

    barrier = pltpu.get_barrier_semaphore()

    def greet(target):
        pl.semaphore_signal(
            barrier, inc=1, device_id=target, device_id_type=pl.DeviceIdType.MESH
        )

    for step in range(spans):
        to_span = lax.rem(span + step, spans)

        @pl.when(has_up)
        def _():
            greet(device(to_span, level + 1, core))

        @pl.when(has_down)
        def _():
            greet(device(to_span, level - 1, core))

        if step > 0:
            greet(device(to_span, level, core))
    greet(pair)

    local = [
        pltpu.make_async_copy(source, target, local_sem.at[index])
        for index, (source, target) in enumerate(
            (
                (rotary, rotary_raw),
                (latents, mine),
                (latents.at[span], place(0, span, level, core)),
                (key_up, key_raw),
                (value_up, value_raw),
                (gain, gain_ref),
            )
        )
    ]
    for copy in local:
        copy.start()
    local[0].wait()
    for sequence in range(spans):
        rotary_mine[sequence] = jnp.concatenate(
            [rotary_raw[sequence, :half], rotary_raw[sequence, half:]], axis=1
        )
    place(1, span, level, core)[...] = rotary_mine[span]
    local[1].wait()
    pl.semaphore_wait(
        barrier,
        spans
        + spans * has_up.astype(jnp.int32)
        + spans * has_down.astype(jnp.int32),
    )

    upper = level * 2 >= levels

    def start_towards(towards, steps):
        for step in steps:
            for part in range(2):
                cross(part, step, towards).start()

    def start_adjacent(steps):
        @pl.when(upper)
        def _():
            @pl.when(has_up)
            def _():
                start_towards(1, steps)

            start_towards(-1, steps)

        @pl.when(jnp.logical_not(upper))
        def _():
            @pl.when(has_down)
            def _():
                start_towards(-1, steps)

            start_towards(1, steps)

    if levels > 1:
        start_adjacent(range(1))
        start_adjacent(range(1, spans))
    start_towards(0, range(1, spans))
    for part, own in enumerate((mine, rotary_mine)):
        send(
            part, span, level, own.at[span], pair, pair_sem, pair_got_sem
        ).start()

    local[3].wait()
    wide[...] = key_raw[...].astype(jnp.float32)
    for head in range(heads):
        weight = wide[pl.ds(head, latent, stride=heads), :] if heads > 1 else wide[...]
        key_weights[head * key_size : (head + 1) * key_size, :] = weight.T.astype(
            jnp.bfloat16
        )
    local[4].wait()
    wide[...] = value_raw[...].astype(jnp.float32)
    for head in range(heads):
        weight = wide[pl.ds(head, latent, stride=heads), :] if heads > 1 else wide[...]
        value_weights[:, head * key_size : (head + 1) * key_size] = weight.astype(
            jnp.bfloat16
        )
    local[2].wait()
    local[5].wait()

    def expand(start, count):
        block = rows[pl.ds(pl.multiple_of(start, count), count), :].astype(jnp.float32)
        scale = lax.rsqrt(jnp.mean(block * block, axis=-1, keepdims=True) + 1e-06)
        ready = (block * scale * gain_ref[...]).astype(jnp.bfloat16)
        lanes = pl.ds(pl.multiple_of(start, count), count)
        keys = lax.dot_general(
            key_weights[...],
            ready,
            (((1,), (1,)), ((), ())),
            preferred_element_type=jnp.float32,
        ).astype(jnp.bfloat16)
        packed = turned[
            pl.ds(pl.multiple_of(start // 2, count // 2), count // 2), :
        ].astype(jnp.float32)
        pieces = []
        for first in range(0, count // 2, half):
            piece = packed[first : first + half]
            pieces += [piece, pltpu.roll(piece, rotary_size, 1)]
        shared = jnp.concatenate(pieces, axis=0).T[:rotary_size].astype(jnp.bfloat16)
        for head in range(heads):
            keys_out[head, :key_size, lanes] = keys[
                head * key_size : (head + 1) * key_size
            ]
            keys_out[head, key_size:, lanes] = shared
        values = jnp.dot(
            ready, value_weights[...], preferred_element_type=jnp.float32
        )
        if heads > 1:
            for head in range(heads):
                mixed[pl.ds(head, count, stride=heads), :] = values[
                    :, head * key_size : (head + 1) * key_size
                ]
            values = mixed[...]
        values_out[
            pl.ds(pl.multiple_of(start * heads, count * heads), count * heads), :
        ] = values.astype(jnp.bfloat16)

    chunk = mixed.shape[0] // heads
    early = chunk == CORES * length

    def finish(origin, plane):
        pair_arrived(origin, plane)
        if early:
            expand(first_row(origin, plane), chunk)

    def origin_of(step):
        return lax.rem(span + step, spans)

    def own_turn(step):
        return (step >= spans) & (step < 2 * spans)

    def pass_on(step, _):
        away = 1 + step // spans
        origin = origin_of(lax.rem(step, spans))
        for plane, exists, more, target, sem in (
            (level - away, level >= away, has_up, above, up_sem),
            (level + away, level + away < levels, has_down, below, down_sem),
        ):

            @pl.when(exists)
            def _():
                for part in range(2):
                    arrived(part, origin, plane)

                    @pl.when(more)
                    def _():
                        send(part, origin, plane, None, target, sem, got_sem).start()

                for part in range(2):
                    send(part, origin, plane, None, pair, pair_sem, pair_got_sem).start()

        @pl.when(own_turn(step) & (step > spans))
        def _():
            for part in range(2):
                arrived(part, origin, level)
                send(part, origin, level, None, pair, pair_sem, pair_got_sem).start()

        @pl.when(step > 0)
        def _():
            finish_step(step - 1)

        return 0

    def finish_step(step):
        away = 1 + step // spans
        origin = origin_of(lax.rem(step, spans))
        for plane, exists in (
            (level - away, level >= away),
            (level + away, level + away < levels),
            (level, own_turn(step)),
        ):

            @pl.when(exists)
            def _():
                finish(origin, plane)

    steps = max(levels - 1, 2) * spans
    lax.fori_loop(0, steps, pass_on, 0)
    finish_step(steps - 1)

    if not early:

        def late(step, _):
            expand(step * chunk, chunk)
            return 0

        lax.fori_loop(0, rows.shape[0] // chunk, late, 0)

    def drain(slot, _):
        origin, plane = slot // levels, slot % levels
        for part in range(2):

            @pl.when(has_up & (plane < level))
            def _():
                send(part, origin, plane, None, above, up_sem, got_sem).wait_send()

            @pl.when(has_down & (plane > level))
            def _():
                send(part, origin, plane, None, below, down_sem, got_sem).wait_send()

            send(part, origin, plane, None, pair, pair_sem, pair_got_sem).wait_send()
        return 0

    lax.fori_loop(0, spans * levels, drain, 0)
    for step in range(spans):
        for part in range(2):

            @pl.when(has_up)
            def _():
                cross(part, step, 1).wait_send()

            @pl.when(has_down)
            def _():
                cross(part, step, -1).wait_send()

            if step > 0:
                cross(part, step, 0).wait_send()


def shards(spans, levels, latents, rotary_rows, latent_gain, key_up, value_up):
    sequences, length, latent = latents.shape
    rotary_size = rotary_rows.shape[2]
    heads, key_size = key_up.shape[1:]
    total = spans * levels * CORES * length
    chunk = max(CORES * length, LANES)
    vmem = pl.BlockSpec(memory_space=pltpu.VMEM)
    hbm = pl.BlockSpec(memory_space=pltpu.HBM)
    slots = spans * levels
    kept = 2 * total * heads * (2 * key_size + rotary_size)
    sems = pltpu.SemaphoreType.DMA
    keys, values = pl.pallas_call(
        functools.partial(gather_expand, spans, levels),
        out_shape=(
            jax.ShapeDtypeStruct((heads, key_size + rotary_size, total), jnp.bfloat16),
            jax.ShapeDtypeStruct((total * heads, key_size), jnp.bfloat16),
        ),
        in_specs=[hbm] * 5,
        out_specs=(vmem, vmem),
        scratch_shapes=[
            pltpu.VMEM(latents.shape, jnp.bfloat16),
            pltpu.VMEM(rotary_rows.shape, jnp.bfloat16),
            pltpu.VMEM((sequences, length // 2, 2 * rotary_size), jnp.bfloat16),
            pltpu.VMEM((total, latent), jnp.bfloat16),
            pltpu.VMEM((total // 2, 2 * rotary_size), jnp.bfloat16),
            pltpu.VMEM((1, latent), jnp.float32),
            pltpu.VMEM((latent * heads, key_size), jnp.bfloat16),
            pltpu.VMEM((latent * heads, key_size), jnp.bfloat16),
            pltpu.VMEM((latent * heads, key_size), jnp.float32),
            pltpu.VMEM((heads * key_size, latent), jnp.bfloat16),
            pltpu.VMEM((latent, heads * key_size), jnp.bfloat16),
            pltpu.VMEM((chunk * heads, key_size), jnp.float32),
            sems((6,)),
            sems((3, spans, 2)),
            sems((slots, 2)),
            sems((slots, 2)),
            sems((slots, 2)),
            sems((slots, 2)),
            sems((slots, 2)),
        ],
        compiler_params=pltpu.CompilerParams(
            collective_id=0, has_side_effects=True, vmem_limit_bytes=40 * 1024 * 1024
        ),
    )(
        latents,
        rotary_rows,
        latent_gain.reshape(1, latent),
        key_up.reshape(latent * heads, key_size),
        value_up.reshape(latent * heads, key_size),
    )
    return keys[None], values.reshape(1, total, heads, key_size)


def solution(mesh):
    placed = (
        P(None, ("span", "model"), None),
        P(None, ("span", "model"), None),
        P(),
        P(None, "model", None),
        P(None, "model", None),
    )
    spans, levels = mesh.shape["span"], mesh.shape["model"] // CORES
    return jax.shard_map(
        functools.partial(shards, spans, levels),
        mesh=mesh,
        in_specs=placed,
        out_specs=(P("span", "model", None, None), P("span", None, "model", None)),
        check_vma=False,
    )
```

```python
import functools

import jax
import jax.numpy as jnp
from jax import lax
from jax.experimental import pallas as pl
from jax.experimental.pallas import tpu as pltpu
from jax.sharding import PartitionSpec as P

CORES = 2
LANES = 128


def gather_expand(
    spans,
    levels,
    latents,
    rotary,
    gain,
    key_up,
    value_up,
    keys_out,
    values_out,
    mine,
    rotary_raw,
    rotary_mine,
    rows,
    turned,
    gain_ref,
    key_raw,
    value_raw,
    wide,
    key_weights,
    value_weights,
    mixed,
    local_sem,
    cross_sem,
    up_sem,
    down_sem,
    pair_sem,
    got_sem,
    pair_got_sem,
):
    span = lax.axis_index("span")
    model = lax.axis_index("model")
    level, core = model // CORES, model % CORES
    length, latent = latents.shape[1], latents.shape[2]
    rotary_size = rotary.shape[2]
    half = length // 2
    heads, key_size = keys_out.shape[0], wide.shape[1]
    has_up, has_down = level < levels - 1, level > 0

    def device(to_span, to_level, to_core):
        return {"span": to_span, "model": to_level * CORES + to_core}

    above = device(span, level + 1, core)
    below = device(span, level - 1, core)
    pair = device(span, level, 1 - core)

    def first_row(origin, plane):
        return (origin * levels + plane) * (CORES * length)

    def place(part, origin, plane, of_core):
        start = first_row(origin, plane) + of_core * length
        if part == 0:
            return rows.at[pl.ds(pl.multiple_of(start, length), length)]
        return turned.at[pl.ds(pl.multiple_of(start // 2, half), half)]

    def send(part, origin, plane, source, target, send_sem, recv_sem):
        slot = origin * levels + plane
        here = place(part, origin, plane, core)
        return pltpu.make_async_remote_copy(
            src_ref=here if source is None else source,
            dst_ref=here,
            send_sem=send_sem.at[slot, part],
            recv_sem=recv_sem.at[slot, part],
            device_id=target,
            device_id_type=pl.DeviceIdType.MESH,
        )

    def cross(part, step, towards):
        to_span = lax.rem(span + (spans - step), spans)
        source = mine if part == 0 else rotary_mine
        return pltpu.make_async_remote_copy(
            src_ref=source.at[to_span],
            dst_ref=place(part, span, level, core),
            send_sem=cross_sem.at[towards + 1, step, part],
            recv_sem=got_sem.at[span * levels + level, part],
            device_id=device(to_span, level + towards, core),
            device_id_type=pl.DeviceIdType.MESH,
        )

    def arrived(part, origin, plane):
        send(part, origin, plane, None, pair, pair_sem, got_sem).wait_recv()

    def pair_arrived(origin, plane):
        for part in range(2):
            slot = origin * levels + plane
            there = place(part, origin, plane, 1 - core)
            pltpu.make_async_remote_copy(
                src_ref=there,
                dst_ref=there,
                send_sem=pair_sem.at[slot, part],
                recv_sem=pair_got_sem.at[slot, part],
                device_id=pair,
                device_id_type=pl.DeviceIdType.MESH,
            ).wait_recv()

    barrier = pltpu.get_barrier_semaphore()

    def greet(target):
        pl.semaphore_signal(
            barrier, inc=1, device_id=target, device_id_type=pl.DeviceIdType.MESH
        )

    for step in range(spans):
        to_span = lax.rem(span + step, spans)

        @pl.when(has_up)
        def _():
            greet(device(to_span, level + 1, core))

        @pl.when(has_down)
        def _():
            greet(device(to_span, level - 1, core))

        if step > 0:
            greet(device(to_span, level, core))
    greet(pair)

    local = [
        pltpu.make_async_copy(source, target, local_sem.at[index])
        for index, (source, target) in enumerate(
            (
                (rotary, rotary_raw),
                (latents, mine),
                (latents.at[span], place(0, span, level, core)),
                (key_up, key_raw),
                (value_up, value_raw),
                (gain, gain_ref),
            )
        )
    ]
    for copy in local:
        copy.start()
    local[0].wait()
    for sequence in range(spans):
        rotary_mine[sequence] = jnp.concatenate(
            [rotary_raw[sequence, :half], rotary_raw[sequence, half:]], axis=1
        )
    place(1, span, level, core)[...] = rotary_mine[span]
    local[1].wait()
    pl.semaphore_wait(
        barrier,
        spans
        + spans * has_up.astype(jnp.int32)
        + spans * has_down.astype(jnp.int32),
    )

    upper = level * 2 >= levels

    def start_towards(towards, steps):
        for step in steps:
            for part in range(2):
                cross(part, step, towards).start()

    def start_adjacent(steps):
        @pl.when(upper)
        def _():
            @pl.when(has_up)
            def _():
                start_towards(1, steps)

            start_towards(-1, steps)

        @pl.when(jnp.logical_not(upper))
        def _():
            @pl.when(has_down)
            def _():
                start_towards(-1, steps)

            start_towards(1, steps)

    if levels > 1:
        start_adjacent(range(1))
        start_adjacent(range(1, spans))
    start_towards(0, range(1, spans))
    for part, own in enumerate((mine, rotary_mine)):
        send(
            part, span, level, own.at[span], pair, pair_sem, pair_got_sem
        ).start()

    local[3].wait()
    wide[...] = key_raw[...].astype(jnp.float32)
    for head in range(heads):
        weight = wide[pl.ds(head, latent, stride=heads), :] if heads > 1 else wide[...]
        key_weights[head * key_size : (head + 1) * key_size, :] = weight.T.astype(
            jnp.bfloat16
        )
    local[4].wait()
    wide[...] = value_raw[...].astype(jnp.float32)
    for head in range(heads):
        weight = wide[pl.ds(head, latent, stride=heads), :] if heads > 1 else wide[...]
        value_weights[:, head * key_size : (head + 1) * key_size] = weight.astype(
            jnp.bfloat16
        )
    local[2].wait()
    local[5].wait()

    def expand(start, count):
        block = rows[pl.ds(pl.multiple_of(start, count), count), :].astype(jnp.float32)
        scale = lax.rsqrt(jnp.mean(block * block, axis=-1, keepdims=True) + 1e-06)
        ready = (block * scale * gain_ref[...]).astype(jnp.bfloat16)
        lanes = pl.ds(pl.multiple_of(start, count), count)
        keys = lax.dot_general(
            key_weights[...],
            ready,
            (((1,), (1,)), ((), ())),
            preferred_element_type=jnp.float32,
        ).astype(jnp.bfloat16)
        packed = turned[
            pl.ds(pl.multiple_of(start // 2, count // 2), count // 2), :
        ].astype(jnp.float32)
        pieces = []
        for first in range(0, count // 2, half):
            piece = packed[first : first + half]
            pieces += [piece, pltpu.roll(piece, rotary_size, 1)]
        shared = jnp.concatenate(pieces, axis=0).T[:rotary_size].astype(jnp.bfloat16)
        for head in range(heads):
            keys_out[head, :key_size, lanes] = keys[
                head * key_size : (head + 1) * key_size
            ]
            keys_out[head, key_size:, lanes] = shared
        values = jnp.dot(
            ready, value_weights[...], preferred_element_type=jnp.float32
        )
        if heads > 1:
            for head in range(heads):
                mixed[pl.ds(head, count, stride=heads), :] = values[
                    :, head * key_size : (head + 1) * key_size
                ]
            values = mixed[...]
        values_out[
            pl.ds(pl.multiple_of(start * heads, count * heads), count * heads), :
        ] = values.astype(jnp.bfloat16)

    chunk = mixed.shape[0] // heads
    early = chunk == CORES * length

    def finish(origin, plane):
        pair_arrived(origin, plane)
        if early:
            expand(first_row(origin, plane), chunk)

    def origin_of(step):
        return lax.rem(span + step, spans)

    def own_turn(step):
        return (step >= spans) & (step < 2 * spans)

    def pass_on(step, _):
        away = 1 + step // spans
        origin = origin_of(lax.rem(step, spans))
        for plane, exists, more, target, sem in (
            (level - away, level >= away, has_up, above, up_sem),
            (level + away, level + away < levels, has_down, below, down_sem),
        ):

            @pl.when(exists)
            def _():
                for part in range(2):
                    arrived(part, origin, plane)

                    @pl.when(more)
                    def _():
                        send(part, origin, plane, None, target, sem, got_sem).start()

                for part in range(2):
                    send(part, origin, plane, None, pair, pair_sem, pair_got_sem).start()

        @pl.when(own_turn(step) & (step > spans))
        def _():
            for part in range(2):
                arrived(part, origin, level)
                send(part, origin, level, None, pair, pair_sem, pair_got_sem).start()

        @pl.when(step > 0)
        def _():
            finish_step(step - 1)

        return 0

    def finish_step(step):
        away = 1 + step // spans
        origin = origin_of(lax.rem(step, spans))
        for plane, exists in (
            (level - away, level >= away),
            (level + away, level + away < levels),
            (level, own_turn(step)),
        ):

            @pl.when(exists)
            def _():
                finish(origin, plane)

    steps = max(levels - 1, 2) * spans
    lax.fori_loop(0, steps, pass_on, 0)
    finish_step(steps - 1)

    if not early:

        def late(step, _):
            expand(step * chunk, chunk)
            return 0

        lax.fori_loop(0, rows.shape[0] // chunk, late, 0)

    def drain(slot, _):
        origin, plane = slot // levels, slot % levels
        for part in range(2):

            @pl.when(has_up & (plane < level))
            def _():
                send(part, origin, plane, None, above, up_sem, got_sem).wait_send()

            @pl.when(has_down & (plane > level))
            def _():
                send(part, origin, plane, None, below, down_sem, got_sem).wait_send()

            send(part, origin, plane, None, pair, pair_sem, pair_got_sem).wait_send()
        return 0

    lax.fori_loop(0, spans * levels, drain, 0)
    for step in range(spans):
        for part in range(2):

            @pl.when(has_up)
            def _():
                cross(part, step, 1).wait_send()

            @pl.when(has_down)
            def _():
                cross(part, step, -1).wait_send()

            if step > 0:
                cross(part, step, 0).wait_send()


def shards(spans, levels, latents, rotary_rows, latent_gain, key_up, value_up):
    sequences, length, latent = latents.shape
    rotary_size = rotary_rows.shape[2]
    heads, key_size = key_up.shape[1:]
    total = spans * levels * CORES * length
    chunk = max(CORES * length, LANES)
    vmem = pl.BlockSpec(memory_space=pltpu.VMEM)
    hbm = pl.BlockSpec(memory_space=pltpu.HBM)
    slots = spans * levels
    sems = pltpu.SemaphoreType.DMA
    keys, values = pl.pallas_call(
        functools.partial(gather_expand, spans, levels),
        out_shape=(
            pltpu.VMEM((heads, key_size + rotary_size, total), jnp.bfloat16),
            pltpu.VMEM((total * heads, key_size), jnp.bfloat16),
        ),
        in_specs=[hbm] * 5,
        out_specs=(vmem, vmem),
        scratch_shapes=[
            pltpu.VMEM(latents.shape, jnp.bfloat16),
            pltpu.VMEM(rotary_rows.shape, jnp.bfloat16),
            pltpu.VMEM((sequences, length // 2, 2 * rotary_size), jnp.bfloat16),
            pltpu.VMEM((total, latent), jnp.bfloat16),
            pltpu.VMEM((total // 2, 2 * rotary_size), jnp.bfloat16),
            pltpu.VMEM((1, latent), jnp.float32),
            pltpu.VMEM((latent * heads, key_size), jnp.bfloat16),
            pltpu.VMEM((latent * heads, key_size), jnp.bfloat16),
            pltpu.VMEM((latent * heads, key_size), jnp.float32),
            pltpu.VMEM((heads * key_size, latent), jnp.bfloat16),
            pltpu.VMEM((latent, heads * key_size), jnp.bfloat16),
            pltpu.VMEM((chunk * heads, key_size), jnp.float32),
            sems((6,)),
            sems((3, spans, 2)),
            sems((slots, 2)),
            sems((slots, 2)),
            sems((slots, 2)),
            sems((slots, 2)),
            sems((slots, 2)),
        ],
        compiler_params=pltpu.CompilerParams(
            collective_id=0, has_side_effects=True, vmem_limit_bytes=40 * 1024 * 1024
        ),
    )(
        *(
            pltpu.with_memory_space_constraint(operand, pltpu.HBM)
            for operand in (
                latents,
                rotary_rows,
                latent_gain.reshape(1, latent),
                key_up.reshape(latent * heads, key_size),
                value_up.reshape(latent * heads, key_size),
            )
        )
    )
    return keys[None], values.reshape(1, total, heads, key_size)


def solution(mesh):
    placed = (
        P(None, ("span", "model"), None),
        P(None, ("span", "model"), None),
        P(),
        P(None, "model", None),
        P(None, "model", None),
    )
    spans, levels = mesh.shape["span"], mesh.shape["model"] // CORES
    return jax.shard_map(
        functools.partial(shards, spans, levels),
        mesh=mesh,
        in_specs=placed,
        out_specs=(P("span", "model", None, None), P("span", None, "model", None)),
        check_vma=False,
    )
```

```python
import functools

import jax
import jax.numpy as jnp
from jax import lax
from jax.experimental import pallas as pl
from jax.experimental.pallas import tpu as pltpu
from jax.sharding import PartitionSpec as P

CORES = 2
LANES = 128


def gather_expand(
    spans,
    levels,
    latents,
    rotary,
    gain,
    key_up,
    value_up,
    keys_out,
    values_out,
    mine,
    rotary_raw,
    rotary_mine,
    rows,
    turned,
    gain_ref,
    key_raw,
    value_raw,
    wide,
    key_weights,
    value_weights,
    mixed,
    local_sem,
    cross_sem,
    up_sem,
    down_sem,
    pair_sem,
    got_sem,
    pair_got_sem,
):
    span = lax.axis_index("span")
    model = lax.axis_index("model")
    level, core = model // CORES, model % CORES
    length, latent = latents.shape[1], latents.shape[2]
    rotary_size = rotary.shape[2]
    half = length // 2
    heads, key_size = keys_out.shape[0], wide.shape[1]
    has_up, has_down = level < levels - 1, level > 0

    def device(to_span, to_level, to_core):
        return {"span": to_span, "model": to_level * CORES + to_core}

    above = device(span, level + 1, core)
    below = device(span, level - 1, core)
    pair = device(span, level, 1 - core)

    def first_row(origin, plane):
        return (origin * levels + plane) * (CORES * length)

    def place(part, origin, plane, of_core):
        start = first_row(origin, plane) + of_core * length
        if part == 0:
            return rows.at[pl.ds(pl.multiple_of(start, length), length)]
        return turned.at[pl.ds(pl.multiple_of(start // 2, half), half)]

    def send(part, origin, plane, source, target, send_sem, recv_sem):
        slot = origin * levels + plane
        here = place(part, origin, plane, core)
        return pltpu.make_async_remote_copy(
            src_ref=here if source is None else source,
            dst_ref=here,
            send_sem=send_sem.at[slot, part],
            recv_sem=recv_sem.at[slot, part],
            device_id=target,
            device_id_type=pl.DeviceIdType.MESH,
        )

    def cross(part, step, towards):
        to_span = lax.rem(span + (spans - step), spans)
        source = mine if part == 0 else rotary_mine
        return pltpu.make_async_remote_copy(
            src_ref=source.at[to_span],
            dst_ref=place(part, span, level, core),
            send_sem=cross_sem.at[towards + 1, step, part],
            recv_sem=got_sem.at[span * levels + level, part],
            device_id=device(to_span, level + towards, core),
            device_id_type=pl.DeviceIdType.MESH,
        )

    def arrived(part, origin, plane):
        send(part, origin, plane, None, pair, pair_sem, got_sem).wait_recv()

    def pair_arrived(origin, plane):
        for part in range(2):
            slot = origin * levels + plane
            there = place(part, origin, plane, 1 - core)
            pltpu.make_async_remote_copy(
                src_ref=there,
                dst_ref=there,
                send_sem=pair_sem.at[slot, part],
                recv_sem=pair_got_sem.at[slot, part],
                device_id=pair,
                device_id_type=pl.DeviceIdType.MESH,
            ).wait_recv()

    barrier = pltpu.get_barrier_semaphore()

    def greet(target):
        pl.semaphore_signal(
            barrier, inc=1, device_id=target, device_id_type=pl.DeviceIdType.MESH
        )

    for step in range(spans):
        to_span = lax.rem(span + step, spans)

        @pl.when(has_up)
        def _():
            greet(device(to_span, level + 1, core))

        @pl.when(has_down)
        def _():
            greet(device(to_span, level - 1, core))

        if step > 0:
            greet(device(to_span, level, core))
    greet(pair)

    local = [
        pltpu.make_async_copy(source, target, local_sem.at[index])
        for index, (source, target) in enumerate(
            (
                (rotary, rotary_raw),
                (latents, mine),
                (latents.at[span], place(0, span, level, core)),
                (key_up, key_raw),
                (value_up, value_raw),
                (gain, gain_ref),
            )
        )
    ]
    for copy in local:
        copy.start()
    local[0].wait()
    for sequence in range(spans):
        rotary_mine[sequence] = jnp.concatenate(
            [rotary_raw[sequence, :half], rotary_raw[sequence, half:]], axis=1
        )
    place(1, span, level, core)[...] = rotary_mine[span]
    local[1].wait()
    pl.semaphore_wait(
        barrier,
        spans
        + spans * has_up.astype(jnp.int32)
        + spans * has_down.astype(jnp.int32),
    )

    upper = level * 2 >= levels

    def start_towards(towards, steps):
        for step in steps:
            for part in range(2):
                cross(part, step, towards).start()

    def start_adjacent(steps):
        @pl.when(upper)
        def _():
            @pl.when(has_up)
            def _():
                start_towards(1, steps)

            start_towards(-1, steps)

        @pl.when(jnp.logical_not(upper))
        def _():
            @pl.when(has_down)
            def _():
                start_towards(-1, steps)

            start_towards(1, steps)

    if levels > 1:
        start_adjacent(range(1))
        start_adjacent(range(1, spans))
    start_towards(0, range(1, spans))
    for part, own in enumerate((mine, rotary_mine)):
        send(
            part, span, level, own.at[span], pair, pair_sem, pair_got_sem
        ).start()

    local[3].wait()
    wide[...] = key_raw[...].astype(jnp.float32)
    for head in range(heads):
        weight = wide[pl.ds(head, latent, stride=heads), :] if heads > 1 else wide[...]
        key_weights[head * key_size : (head + 1) * key_size, :] = weight.T.astype(
            jnp.bfloat16
        )
    local[4].wait()
    wide[...] = value_raw[...].astype(jnp.float32)
    for head in range(heads):
        weight = wide[pl.ds(head, latent, stride=heads), :] if heads > 1 else wide[...]
        value_weights[:, head * key_size : (head + 1) * key_size] = weight.astype(
            jnp.bfloat16
        )
    local[2].wait()
    local[5].wait()

    def expand(start, count):
        block = rows[pl.ds(pl.multiple_of(start, count), count), :].astype(jnp.float32)
        scale = lax.rsqrt(jnp.mean(block * block, axis=-1, keepdims=True) + 1e-06)
        ready = (block * scale * gain_ref[...]).astype(jnp.bfloat16)
        lanes = pl.ds(pl.multiple_of(start, count), count)
        keys = lax.dot_general(
            key_weights[...],
            ready,
            (((1,), (1,)), ((), ())),
            preferred_element_type=jnp.float32,
        ).astype(jnp.bfloat16)
        packed = turned[
            pl.ds(pl.multiple_of(start // 2, count // 2), count // 2), :
        ].astype(jnp.float32)
        pieces = []
        for first in range(0, count // 2, half):
            piece = packed[first : first + half]
            pieces += [piece, pltpu.roll(piece, rotary_size, 1)]
        shared = jnp.concatenate(pieces, axis=0).T[:rotary_size].astype(jnp.bfloat16)
        for head in range(heads):
            keys_out[head, :key_size, lanes] = keys[
                head * key_size : (head + 1) * key_size
            ]
            keys_out[head, key_size:, lanes] = shared
        values = jnp.dot(
            ready, value_weights[...], preferred_element_type=jnp.float32
        )
        if heads > 1:
            for head in range(heads):
                mixed[pl.ds(head, count, stride=heads), :] = values[
                    :, head * key_size : (head + 1) * key_size
                ]
            values = mixed[...]
        values_out[
            pl.ds(pl.multiple_of(start * heads, count * heads), count * heads), :
        ] = values.astype(jnp.bfloat16)

    chunk = mixed.shape[0] // heads
    early = chunk == CORES * length

    def finish(origin, plane):
        pair_arrived(origin, plane)
        if early:
            expand(first_row(origin, plane), chunk)

    def origin_of(step):
        return lax.rem(span + step, spans)

    def own_turn(step):
        return (step >= spans) & (step < 2 * spans)

    def pass_on(step, _):
        away = 1 + step // spans
        origin = origin_of(lax.rem(step, spans))
        for plane, exists, more, target, sem in (
            (level - away, level >= away, has_up, above, up_sem),
            (level + away, level + away < levels, has_down, below, down_sem),
        ):

            @pl.when(exists)
            def _():
                for part in range(2):
                    arrived(part, origin, plane)

                    @pl.when(more)
                    def _():
                        send(part, origin, plane, None, target, sem, got_sem).start()

                for part in range(2):
                    send(part, origin, plane, None, pair, pair_sem, pair_got_sem).start()

        @pl.when(own_turn(step) & (step > spans))
        def _():
            for part in range(2):
                arrived(part, origin, level)
                send(part, origin, level, None, pair, pair_sem, pair_got_sem).start()

        @pl.when(step > 0)
        def _():
            finish_step(step - 1)

        return 0

    def finish_step(step):
        away = 1 + step // spans
        origin = origin_of(lax.rem(step, spans))
        for plane, exists in (
            (level - away, level >= away),
            (level + away, level + away < levels),
            (level, own_turn(step)),
        ):

            @pl.when(exists)
            def _():
                finish(origin, plane)

    steps = max(levels - 1, 2) * spans
    lax.fori_loop(0, steps, pass_on, 0)
    finish_step(steps - 1)

    if not early:

        def late(step, _):
            expand(step * chunk, chunk)
            return 0

        lax.fori_loop(0, rows.shape[0] // chunk, late, 0)

    def drain(slot, _):
        origin, plane = slot // levels, slot % levels
        for part in range(2):

            @pl.when(has_up & (plane < level))
            def _():
                send(part, origin, plane, None, above, up_sem, got_sem).wait_send()

            @pl.when(has_down & (plane > level))
            def _():
                send(part, origin, plane, None, below, down_sem, got_sem).wait_send()

            send(part, origin, plane, None, pair, pair_sem, pair_got_sem).wait_send()
        return 0

    lax.fori_loop(0, spans * levels, drain, 0)
    for step in range(spans):
        for part in range(2):

            @pl.when(has_up)
            def _():
                cross(part, step, 1).wait_send()

            @pl.when(has_down)
            def _():
                cross(part, step, -1).wait_send()

            if step > 0:
                cross(part, step, 0).wait_send()


def store(keys_in, values_in, keys_out, values_out, sems):
    copies = [
        pltpu.make_async_copy(keys_in, keys_out, sems.at[0]),
        pltpu.make_async_copy(values_in, values_out, sems.at[1]),
    ]
    for copy in copies:
        copy.start()
    for copy in copies:
        copy.wait()


def shards(spans, levels, latents, rotary_rows, latent_gain, key_up, value_up):
    sequences, length, latent = latents.shape
    rotary_size = rotary_rows.shape[2]
    heads, key_size = key_up.shape[1:]
    total = spans * levels * CORES * length
    chunk = max(CORES * length, LANES)
    vmem = pl.BlockSpec(memory_space=pltpu.VMEM)
    hbm = pl.BlockSpec(memory_space=pltpu.HBM)
    slots = spans * levels
    sems = pltpu.SemaphoreType.DMA
    keys, values = pl.pallas_call(
        functools.partial(gather_expand, spans, levels),
        out_shape=(
            pltpu.VMEM((heads, key_size + rotary_size, total), jnp.bfloat16),
            pltpu.VMEM((total * heads, key_size), jnp.bfloat16),
        ),
        in_specs=[hbm] * 5,
        out_specs=(vmem, vmem),
        scratch_shapes=[
            pltpu.VMEM(latents.shape, jnp.bfloat16),
            pltpu.VMEM(rotary_rows.shape, jnp.bfloat16),
            pltpu.VMEM((sequences, length // 2, 2 * rotary_size), jnp.bfloat16),
            pltpu.VMEM((total, latent), jnp.bfloat16),
            pltpu.VMEM((total // 2, 2 * rotary_size), jnp.bfloat16),
            pltpu.VMEM((1, latent), jnp.float32),
            pltpu.VMEM((latent * heads, key_size), jnp.bfloat16),
            pltpu.VMEM((latent * heads, key_size), jnp.bfloat16),
            pltpu.VMEM((latent * heads, key_size), jnp.float32),
            pltpu.VMEM((heads * key_size, latent), jnp.bfloat16),
            pltpu.VMEM((latent, heads * key_size), jnp.bfloat16),
            pltpu.VMEM((chunk * heads, key_size), jnp.float32),
            sems((6,)),
            sems((3, spans, 2)),
            sems((slots, 2)),
            sems((slots, 2)),
            sems((slots, 2)),
            sems((slots, 2)),
            sems((slots, 2)),
        ],
        compiler_params=pltpu.CompilerParams(
            collective_id=0, has_side_effects=True, vmem_limit_bytes=40 * 1024 * 1024
        ),
    )(
        *(
            pltpu.with_memory_space_constraint(operand, pltpu.HBM)
            for operand in (
                latents,
                rotary_rows,
                latent_gain.reshape(1, latent),
                key_up.reshape(latent * heads, key_size),
                value_up.reshape(latent * heads, key_size),
            )
        )
    )
    keys, values = pl.pallas_call(
        store,
        out_shape=tuple(
            jax.ShapeDtypeStruct(part.shape, part.dtype) for part in (keys, values)
        ),
        in_specs=[vmem, vmem],
        out_specs=(hbm, hbm),
        scratch_shapes=[sems((2,))],
        compiler_params=pltpu.CompilerParams(vmem_limit_bytes=4 * 1024 * 1024),
    )(
        pltpu.with_memory_space_constraint(keys, pltpu.VMEM),
        pltpu.with_memory_space_constraint(values, pltpu.VMEM),
    )
    return keys[None], values.reshape(1, total, heads, key_size)


def solution(mesh):
    placed = (
        P(None, ("span", "model"), None),
        P(None, ("span", "model"), None),
        P(),
        P(None, "model", None),
        P(None, "model", None),
    )
    spans, levels = mesh.shape["span"], mesh.shape["model"] // CORES
    return jax.shard_map(
        functools.partial(shards, spans, levels),
        mesh=mesh,
        in_specs=placed,
        out_specs=(P("span", "model", None, None), P("span", None, "model", None)),
        check_vma=False,
    )
```
